256 devices in a mesh: seq: 16 (over y_hi, z), head: 16 (over y_lo, x, core).
Axes of the slice: x: 4, y: 4 (y_hi: 2, y_lo: 2; y = y_hi * 2 + y_lo), z: 8, core: 2. Of those that a mesh axis runs over, the one named last changes fastest.
Arguments:
- queries: bfloat16 [16384, 4096], P(('seq', 'head')), may hold values from -9 to 9, as said below
- keys: bfloat16 [16384, 512], P(('seq', 'head')), may hold values from -9 to 9, as said below
- values: bfloat16 [16384, 512], P(('seq', 'head')), may hold values from -6 to 6
Outputs:
- attended: bfloat16 [16384, 4096], P(('seq', 'head'))
The draws below stay inside these ranges and needn't reach their ends.
Inputs may be any that keep to these rules, and one draw needn't show every extreme that they name: `queries`: query entries are of order one except on a few rows. `keys`: key entries are of order one except on a few rows.
All inputs are finite; a program needn't handle non-finite values.
Results may differ from the reference program's by a relative error of at most 0.005.
Values may be sent and summed in bfloat16 or wider, within the bound.
A program may use at most 64 MiB of HBM per device.

```python
import math
import jax
import jax.numpy as jnp
from jax import lax

H = 32
KV = 4
DH = 128
TOKENS = 16384


def paired(key):
    base = jax.random.fold_in(key, 7)
    key_q, key_k = jax.random.split(base, 2)
    query_mat = jnp.clip(jax.random.normal(key_q, (TOKENS, H * DH), jnp.float32), -6.0, 6.0)
    key_mat = jnp.clip(jax.random.normal(key_k, (TOKENS, KV * DH), jnp.float32), -6.0, 6.0)
    return (query_mat, key_mat)


def draw_queries(key, part):
    return paired(key)[0].astype(jnp.bfloat16)


def draw_keys(key, part):
    return paired(key)[1].astype(jnp.bfloat16)


def shard_levels(key, dims, pieces, smallest, high):
    factor_of, own = 1.0, jax.random.fold_in(key, 6)
    for position, shards_of in pieces:
        draws = jnp.exp(jax.random.uniform(jax.random.fold_in(own, position), (shards_of,), jnp.float32, smallest / len(pieces), high / len(pieces)))
        factor_of = factor_of * jnp.repeat(draws, dims[position] // shards_of).reshape([-1 if axis == position else 1 for axis in range(len(dims))])
    return factor_of


def scatter_about(rng, dims, spread, bound, shards=(), kind=jnp.bfloat16):
    array = spread * jax.random.normal(rng, dims, jnp.float32)
    if shards:
        array = array * shard_levels(rng, dims, shards, -0.22, 0.18)
    return jnp.clip(array, -bound, bound).astype(kind)


def setup_inputs(seed: int = 0) -> dict:
    seeds = jax.random.split(jax.random.key(seed), 4)
    queries = draw_queries(jax.random.fold_in(seeds[3], 71), 0)
    keys = draw_keys(jax.random.fold_in(seeds[3], 71), 0)
    values = scatter_about(seeds[2], (TOKENS, KV * DH), 1.0, 6.0, ((0, 256),))
    return dict(queries=queries, keys=keys, values=values)


def reference(queries, keys, values):
    length = queries.shape[0]
    block = min(1024, length)
    blocks = length // block
    group = H // KV
    scale = 1.0 / math.sqrt(DH)
    q_heads = queries.reshape(length, H, DH)
    k_heads = keys.reshape(length, KV, DH)
    v_heads = values.reshape(length, KV, DH)
    key_pos = jnp.arange(length, dtype=jnp.int32)

    def one_head(head):
        q_mat = lax.dynamic_index_in_dim(q_heads, head, 1, keepdims=False)
        k_mat = lax.dynamic_index_in_dim(k_heads, head // group, 1, keepdims=False)
        v_mat = lax.dynamic_index_in_dim(v_heads, head // group, 1, keepdims=False)

        def one_block(index):
            first = (index * block).astype(jnp.int32)
            rows = lax.dynamic_slice_in_dim(q_mat, first, block, 0)
            scores = jnp.dot(rows, k_mat.T, preferred_element_type=jnp.float32) * scale
            query_pos = first + jnp.arange(block, dtype=jnp.int32)
            scores = jnp.where(key_pos[None, :] <= query_pos[:, None], scores, -jnp.inf)
            rowmax = lax.optimization_barrier(jnp.max(scores, axis=1, keepdims=True))
            expo = jnp.exp(scores - rowmax)
            total = lax.optimization_barrier(jnp.sum(expo, axis=1, keepdims=True))
            numer = jnp.dot(expo.astype(jnp.bfloat16), v_mat, preferred_element_type=jnp.float32)
            return (numer / total).astype(jnp.bfloat16)
        return lax.map(one_block, jnp.arange(blocks, dtype=jnp.int32)).reshape(length, DH)
    result = lax.map(one_head, jnp.arange(H, dtype=jnp.int32))
    return result.transpose(1, 0, 2).reshape(length, H * DH)
```

```python
import functools
import math

import jax
import jax.numpy as jnp
from jax import lax
from jax.experimental import pallas as pl
from jax.experimental.pallas import tpu as pltpu
from jax.sharding import PartitionSpec as P

H = 32
KV = 4
DH = 128
NX, NY, NZ, NC = 4, 4, 8, 2
TOK = 64
REP = H // KV
COLS = REP * DH
NQ = REP * TOK
CHUNK = NX * NC * 2 * TOK
LOGICAL = pl.DeviceIdType.MESH
NEG = -1e30
FACTOR = math.log2(math.e) / math.sqrt(DH)


def device(x, y, z, c):
    return ((y // 2) * NZ + z, (y % 2) * (NX * NC) + x * NC + c)


def kernel(
    q_hbm, k_hbm, v_hbm, out_hbm,
    kbuf, vbuf, vloc, qin, qt, m_ref, l_ref, o_ref, s_ref, obuf,
    send0, recv0k, recv0v, sendq, recvq,
    sendx, recvx, sendz, recvz, sendd, recvd, sendo, recvo, local_sem,
):
    seq, head = lax.axis_index("seq"), lax.axis_index("head")
    yh, z = seq // NZ, seq % NZ
    yl, x, c = head // (NX * NC), (head % (NX * NC)) // NC, head % NC
    y = yh * 2 + yl
    mirror = NZ - 1 - z
    partner = device(x, y, z, 1 - c)
    bufs = (kbuf, vbuf)

    def remote(src, dst, send, recv, dev):
        return pltpu.make_async_remote_copy(
            src_ref=src, dst_ref=dst, send_sem=send, recv_sem=recv,
            device_id=dev, device_id_type=LOGICAL,
        )

    barrier = pltpu.get_barrier_semaphore()
    peers = [device(x, (y + d) % NY, z, c) for d in (1, 2, 3)]
    peers += [device(x, (y + d) % NY, mirror, c) for d in range(NY)]
    peers += [device((x + d) % NX, y, z, c) for d in (1, 2, 3)]
    peers += [device(x, y, (z + d) % NZ, c) for d in (1, NZ - 1)]
    peers += [partner]
    for dev in peers:
        pl.semaphore_signal(barrier, inc=1, device_id=dev, device_id_type=LOGICAL)
    pl.semaphore_wait(barrier, len(peers))

    def kv_slice(ref, g):
        return ref.at[:, pl.ds(pl.multiple_of(g * DH, DH), DH)]

    rows = pl.ds(pl.multiple_of(yl * TOK, TOK), TOK)
    first = []
    for d in (1, 3, 2):
        g = (y + d) % NY
        dev = device(x, g, z, c)
        ck = remote(kv_slice(k_hbm, g), kbuf.at[z, c, yh, x, rows], send0.at[0, d], recv0k.at[d], dev)
        cv = remote(kv_slice(v_hbm, g), vloc.at[yh, rows], send0.at[1, d], recv0v.at[d], dev)
        ck.start()
        cv.start()
        first += [(ck, cv)]
    lk = pltpu.make_async_copy(kv_slice(k_hbm, y), kbuf.at[z, c, yh, x, rows], local_sem.at[0])
    lv = pltpu.make_async_copy(kv_slice(v_hbm, y), vloc.at[yh, rows], local_sem.at[1])
    lk.start()
    lv.start()

    def q_slice(ref, g):
        return ref.at[:, pl.ds(pl.multiple_of(g * COLS, COLS), COLS)]

    zd = jnp.where(yh == 0, z, mirror)
    q_copies = [
        remote(q_slice(q_hbm, (y + d) % NY), qin.at[y], sendq.at[d], recvq.at[y], device(x, (y + d) % NY, zd, c))
        for d in range(NY)
    ]
    q_own = pltpu.make_async_copy(q_slice(q_hbm, y), qin.at[y], local_sem.at[2])
    for d in (1, 2, 3):
        q_copies[d].start()

    @pl.when(yh == 1)
    def _():
        q_copies[0].start()

    @pl.when(yh == 0)
    def _():
        q_own.start()

    lk.wait()
    for ck, _ in first:
        ck.wait_recv()
    xs = {}
    for a in (0, 1):
        if a == 1:
            lv.wait()
            for _, cv in first:
                cv.wait_recv()
            for h in (0, 1):
                vbuf[z, c, h, x] = vloc[h].astype(jnp.float32).T.astype(jnp.bfloat16)
        for d in (1, 3, 2):
            part = bufs[a].at[z, c, :, x]
            xs[a, d] = remote(part, part, sendx.at[a, d], recvx.at[a, d], device((x + d) % NX, y, z, c))
            xs[a, d].start()

    for p in range(NY):
        @pl.when(y == p)
        def _(p=p):
            @pl.when(yh == 0)
            def _():
                q_own.wait()

        @pl.when((y != p) | (yh == 1))
        def _(p=p):
            remote(qin.at[p], qin.at[p], sendq.at[0], recvq.at[p], partner).wait_recv()

        stacked = jnp.concatenate([qin[p, :, h * DH:(h + 1) * DH] for h in range(REP)], axis=0)
        scaled = (stacked.astype(jnp.float32) * FACTOR).T
        high = scaled.astype(jnp.bfloat16)
        qt[p, :DH] = high
        qt[p, DH:] = (scaled - high.astype(jnp.float32)).astype(jnp.bfloat16)
    m_ref[...] = jnp.full(m_ref.shape, NEG, jnp.float32)
    l_ref[...] = jnp.zeros(l_ref.shape, jnp.float32)
    o_ref[...] = jnp.zeros(o_ref.shape, jnp.float32)

    right, left = device(x, y, (z + 1) % NZ, c), device(x, y, (z + NZ - 1) % NZ, c)
    started = []

    def hop(a, zz, step, way):
        part = bufs[a].at[zz, c]
        cp = remote(part, part, sendz.at[a, way, step], recvz.at[a, way, step], right if way == 0 else left)
        cp.start()
        started.append(cp)

    def arrived(a, zz, step, way):
        part = bufs[a].at[zz, c]
        remote(part, part, sendz.at[a, way, step], recvz.at[a, way, step], partner).wait_recv()

    def across(a, zz, slot):
        part = bufs[a].at[zz, c]
        cp = remote(part, part, sendd.at[a, slot], recvd.at[a, slot], partner)
        cp.start()
        started.append(cp)

    def crossed(a, zz, slot):
        part = bufs[a].at[zz, 1 - c]
        remote(part, part, sendd.at[a, slot], recvd.at[a, slot], partner).wait_recv()

    def count(zz):
        return 1 + (zz <= z).astype(jnp.int32) + (zz <= mirror).astype(jnp.int32)

    def decode(j, zs):
        n1 = count(zs[0])
        second = (j >= n1).astype(jnp.int32)
        zz = zs[0] + second * (zs[-1] - zs[0])
        jj = j - second * n1
        has_early = (zz <= z).astype(jnp.int32)
        is_early = jnp.where(jj == 1, has_early, 0)
        is_late = jnp.where(jj == 0, 0, 1 - is_early)
        diag = is_early * (zz == z).astype(jnp.int32) + is_late * (zz == mirror).astype(jnp.int32)
        return zz, is_late, 1 - is_early, diag

    def chunk_keys(zz, half):
        k = jnp.concatenate([kbuf[zz, cc, half, xx] for cc in range(NC) for xx in range(NX)], axis=0)
        return jnp.concatenate([k, k], axis=1)

    def chunk_values(zz, half):
        return jnp.concatenate([vbuf[zz, cc, half, xx] for cc in range(NC) for xx in range(NX)], axis=1)

    def score(work, t):
        zz, half, group, _ = work
        s_ref[t] = jnp.dot(chunk_keys(zz, half), qt[group * 2 + t], preferred_element_type=jnp.float32)

    def accumulate(work, t, masked):
        zz, half, group, _ = work
        p = group * 2 + t
        s = s_ref[t]
        if masked:
            r = lax.broadcasted_iota(jnp.int32, (CHUNK, NQ), 0)
            k_pos = ((r >> 6) & 1) * 512 + ((r >> 7) & 3) * 128 + (r >> 9) * 64 + (r & 63)
            q_pos = t * 512 + x * 128 + c * 64 + (lax.broadcasted_iota(jnp.int32, (CHUNK, NQ), 1) & 63)
            s = jnp.where(k_pos <= q_pos, s, NEG)
        m_old = m_ref[p]
        m_new = jnp.maximum(m_old, jnp.max(s, axis=0, keepdims=True))
        alpha = jnp.exp2(m_old - m_new)
        e = jnp.exp2(s - m_new)
        m_ref[p] = m_new
        l_ref[p] = l_ref[p] * alpha + jnp.sum(e, axis=0, keepdims=True)
        pv = jnp.dot(chunk_values(zz, half), e.astype(jnp.bfloat16), preferred_element_type=jnp.float32)
        o_ref[p] = o_ref[p] * alpha + pv

    def attend(zs):
        total = count(zs[0])
        if len(zs) > 1:
            total = total + count(zs[1])
        score(decode(0, zs), 0)

        def body(j, carry):
            work = decode(j, zs)
            after = decode(jnp.minimum(j + 1, total - 1), zs)

            def run(masked):
                score(work, 1)
                accumulate(work, 0, masked)
                score(after, 0)
                accumulate(work, 1, masked)

            @pl.when(work[3] == 0)
            def _():
                run(False)

            @pl.when(work[3] == 1)
            def _():
                run(True)

            return carry

        lax.fori_loop(0, total, body, 0)

    for a in (0, 1):
        for d in (1, 3, 2):
            xs[a, d].wait_recv()
        for way in (0, 1):
            hop(a, z, 0, way)
        across(a, z, 0)
    for a in (0, 1):
        crossed(a, z, 0)
    attend((z,))
    for k in (1, 2, 3):
        low, high = (z + NZ - k) % NZ, (z + k) % NZ
        for a in (0, 1):
            for way, zz in ((0, low), (1, high)):
                arrived(a, zz, k - 1, way)
                if k < 3 or a == way:
                    hop(a, zz, k, way)
                across(a, zz, 2 * k - 1 + way)
        for a in (0, 1):
            for way, zz in ((0, low), (1, high)):
                crossed(a, zz, 2 * k - 1 + way)
        attend((low, high))
    far = (z + 4) % NZ
    for a in (0, 1):
        arrived(a, far, 3, a)
        across(a, far, 7)
    for a in (0, 1):
        crossed(a, far, 7)
    attend((far,))

    def piece(p):
        zp = z if p < 2 else mirror
        return remote(obuf.at[p], q_slice(out_hbm, y), sendo.at[p], recvo.at[y], device(x, p, zp, c))

    own = pltpu.make_async_copy(obuf.at[y], q_slice(out_hbm, y), local_sem.at[3])
    for p in range(NY):
        result = (o_ref[p] / l_ref[p]).T.astype(jnp.bfloat16)
        for h in range(REP):
            obuf[p, :, h * DH:(h + 1) * DH] = result[h * TOK:(h + 1) * TOK]
        if p < 2:
            @pl.when(y == p)
            def _():
                own.start()

            @pl.when(y != p)
            def _(p=p):
                piece(p).start()
        else:
            piece(p).start()

    for d in range(NY):
        g = (y + d) % NY
        landing = remote(obuf.at[0], q_slice(out_hbm, g), sendo.at[0], recvo.at[g], partner)
        if d:
            landing.wait_recv()
        else:
            @pl.when(yh == 1)
            def _():
                landing.wait_recv()

            @pl.when(yh == 0)
            def _():
                own.wait()

    for ck, cv in first:
        ck.wait_send()
        cv.wait_send()
    for d in (1, 2, 3):
        q_copies[d].wait_send()
        for a in (0, 1):
            xs[a, d].wait_send()

    @pl.when(yh == 1)
    def _():
        q_copies[0].wait_send()

    for cp in started:
        cp.wait_send()
    for p in range(NY):
        if p < 2:
            @pl.when(y != p)
            def _(p=p):
                piece(p).wait_send()
        else:
            piece(p).wait_send()


def per_device(queries, keys, values):
    bf16, f32 = jnp.bfloat16, jnp.float32
    dma = pltpu.SemaphoreType.DMA
    return pl.pallas_call(
        kernel,
        out_shape=jax.ShapeDtypeStruct(queries.shape, bf16),
        in_specs=[pl.BlockSpec(memory_space=pltpu.HBM)] * 3,
        out_specs=pl.BlockSpec(memory_space=pltpu.HBM),
        scratch_shapes=[
            pltpu.VMEM((NZ, NC, 2, NX, 2 * TOK, DH), bf16),
            pltpu.VMEM((NZ, NC, 2, NX, DH, 2 * TOK), bf16),
            pltpu.VMEM((2, 2 * TOK, DH), bf16),
            pltpu.VMEM((NY, TOK, COLS), bf16),
            pltpu.VMEM((NY, 2 * DH, NQ), bf16),
            pltpu.VMEM((NY, 1, NQ), f32),
            pltpu.VMEM((NY, 1, NQ), f32),
            pltpu.VMEM((NY, DH, NQ), f32),
            pltpu.VMEM((2, CHUNK, NQ), f32),
            pltpu.VMEM((NY, TOK, COLS), bf16),
            dma((2, 4)), dma((4,)), dma((4,)), dma((4,)), dma((4,)),
            dma((2, 4)), dma((2, 4)), dma((2, 2, 4)), dma((2, 2, 4)),
            dma((2, 8)), dma((2, 8)), dma((4,)), dma((4,)), dma((4,)),
        ],
        compiler_params=pltpu.CompilerParams(
            collective_id=0, has_side_effects=True, vmem_limit_bytes=60 * 2**20
        ),
        name="attention",
    )(queries, keys, values)


def solution(mesh):
    spec = P(("seq", "head"), None)
    return jax.shard_map(
        per_device, mesh=mesh, in_specs=(spec, spec, spec), out_specs=spec, check_vma=False
    )
```

```python
import functools
import math

import jax
import jax.numpy as jnp
from jax import lax
from jax.experimental import pallas as pl
from jax.experimental.pallas import tpu as pltpu
from jax.sharding import PartitionSpec as P

H = 32
KV = 4
DH = 128
NX, NY, NZ, NC = 4, 4, 8, 2
TOK = 64
REP = H // KV
COLS = REP * DH
NQ = REP * TOK
CHUNK = NX * NC * 2 * TOK
LOGICAL = pl.DeviceIdType.MESH
NEG = -1e30
FACTOR = math.log2(math.e) / math.sqrt(DH)


def device(x, y, z, c):
    return ((y // 2) * NZ + z, (y % 2) * (NX * NC) + x * NC + c)


def kernel(
    q_hbm, k_hbm, v_hbm, out_hbm,
    kbuf, vbuf, vloc, qin, qt, m_ref, l_ref, o_ref, s_ref, obuf,
    send0, recv0k, recv0v, sendq, recvq, sendkx, recvkx, sendvx, recvvx,
    sendz, recvz, sendd, recvd, sendo, recvo, local_sem,
):
    seq, head = lax.axis_index("seq"), lax.axis_index("head")
    yh, z = seq // NZ, seq % NZ
    yl, x, c = head // (NX * NC), (head % (NX * NC)) // NC, head % NC
    y = yh * 2 + yl
    partner = device(x, y, z, 1 - c)
    right, left = device(x, y, (z + 1) % NZ, c), device(x, y, (z + NZ - 1) % NZ, c)
    low = [(z + NZ - k) % NZ for k in range(4)]
    high = [(z + k) % NZ for k in range(5)]
    far = high[4]
    started = []

    def remote(src, dst, send, recv, dev):
        return pltpu.make_async_remote_copy(
            src_ref=src, dst_ref=dst, send_sem=send, recv_sem=recv,
            device_id=dev, device_id_type=LOGICAL,
        )

    barrier = pltpu.get_barrier_semaphore()
    peers = [device(x, (y + d) % NY, z, c) for d in (1, 2, 3)]
    peers += [device((x + d) % NX, y, z, c) for d in (1, 2, 3)]
    peers += [right, left, partner]
    for dev in peers:
        pl.semaphore_signal(barrier, inc=1, device_id=dev, device_id_type=LOGICAL)
    pl.semaphore_wait(barrier, len(peers))

    def kv_slice(ref, g):
        return ref.at[:, pl.ds(pl.multiple_of(g * DH, DH), DH)]

    rows = pl.ds(pl.multiple_of(yl * TOK, TOK), TOK)
    first_k, first_v = [], []
    for d in (1, 3, 2):
        g = (y + d) % NY
        dev = device(x, g, z, c)
        first_v.append(remote(kv_slice(v_hbm, g), vloc.at[yh, rows], send0.at[1, d], recv0v.at[d], dev))
        first_k.append(remote(kv_slice(k_hbm, g), kbuf.at[z, c, yh, x, rows], send0.at[0, d], recv0k.at[d], dev))
    own_v = pltpu.make_async_copy(kv_slice(v_hbm, y), vloc.at[yh, rows], local_sem.at[1])
    own_k = pltpu.make_async_copy(kv_slice(k_hbm, y), kbuf.at[z, c, yh, x, rows], local_sem.at[0])
    for cp in first_v + [own_v] + first_k + [own_k]:
        cp.start()

    def q_slice(ref, g):
        return ref.at[:, pl.ds(pl.multiple_of(g * COLS, COLS), COLS)]

    q_copies = [
        remote(q_slice(q_hbm, (y + d) % NY), qin.at[y], sendq.at[d], recvq.at[y], device(x, (y + d) % NY, z, c))
        for d in (1, 3, 2)
    ]
    own_q = pltpu.make_async_copy(q_slice(q_hbm, y), qin.at[y], local_sem.at[2])
    for cp in q_copies + [own_q]:
        cp.start()

    def keys_x(d):
        part = kbuf.at[z, c, :, x]
        return remote(part, part, sendkx.at[d], recvkx.at[d], device((x + d) % NX, y, z, c))

    def values_x(zz, slot, d):
        part = vbuf.at[zz, c, :, x]
        return remote(part, part, sendvx.at[slot, d], recvvx.at[slot, d], device((x + d) % NX, y, z, c))

    def along_z(a, zz, step, way):
        if a == 0:
            part = kbuf.at[zz, c] if step < 3 else kbuf.at[zz, c, way]
        else:
            part = vbuf.at[zz, c, :, x] if step < 3 else vbuf.at[zz, c, way, x]
        return remote(part, part, sendz.at[a, way, step], recvz.at[a, way, step], right if way == 0 else left)

    def across(a, zz, core, slot):
        part = (kbuf, vbuf)[a].at[zz, core]
        return remote(part, part, sendd.at[a, slot], recvd.at[a, slot], partner)

    def go(cp):
        cp.start()
        started.append(cp)

    def spread_values(zz, slot):
        for d in (1, 3, 2):
            go(values_x(zz, slot, d))

    def cross_values(zz, slot):
        for d in (1, 3, 2):
            values_x(zz, slot, d).wait_recv()
        go(across(1, zz, c, slot))

    def crossed(zz, slot):
        for a in (0, 1):
            across(a, zz, 1 - c, slot).wait_recv()

    def advance_values(k):
        if k < 4:
            for way, zz in ((0, low[k]), (1, high[k])):
                along_z(1, zz, k - 1, way).wait_recv()
                go(along_z(1, zz, k, way))
                spread_values(zz, 2 * k - 1 + way)
        else:
            for way in (0, 1):
                along_z(1, far, 3, way).wait_recv()
            spread_values(far, 7)

    def advance_keys(k):
        if k < 4:
            for way, zz in ((0, low[k]), (1, high[k])):
                along_z(0, zz, k - 1, way).wait_recv()
                go(along_z(0, zz, k, way))
                go(across(0, zz, c, 2 * k - 1 + way))
        else:
            for way in (0, 1):
                along_z(0, far, 3, way).wait_recv()
            go(across(0, far, c, 7))

    own_v.wait()
    for cp in first_v:
        cp.wait_recv()
    for h in (0, 1):
        vbuf[z, c, h, x] = vloc[h].astype(jnp.float32).T.astype(jnp.bfloat16)
    own_k.wait()
    for cp in first_k:
        cp.wait_recv()
    for d in (1, 3, 2):
        go(keys_x(d))
    for way in (0, 1):
        go(along_z(1, z, 0, way))
    spread_values(z, 0)

    m_ref[...] = jnp.full(m_ref.shape, NEG, jnp.float32)
    l_ref[...] = jnp.zeros(l_ref.shape, jnp.float32)
    o_ref[...] = jnp.zeros(o_ref.shape, jnp.float32)

    for d in (1, 3, 2):
        keys_x(d).wait_recv()
    for way in (0, 1):
        go(along_z(0, z, 0, way))
    go(across(0, z, c, 0))
    advance_values(1)
    cross_values(z, 0)

    for p in range(NY):
        @pl.when(y == p)
        def _():
            own_q.wait()

        @pl.when(y != p)
        def _(p=p):
            remote(qin.at[p], qin.at[p], sendq.at[0], recvq.at[p], partner).wait_recv()

        stacked = jnp.concatenate([qin[p, :, h * DH:(h + 1) * DH] for h in range(REP)], axis=0)
        scaled = (stacked.astype(jnp.float32) * FACTOR).T
        high_part = scaled.astype(jnp.bfloat16)
        qt[p, :DH] = high_part
        qt[p, DH:] = (scaled - high_part.astype(jnp.float32)).astype(jnp.bfloat16)

    def chunk_keys(zz, half):
        k = jnp.concatenate([kbuf[zz, cc, half, xx] for cc in range(NC) for xx in range(NX)], axis=0)
        return jnp.concatenate([k, k], axis=1)

    def chunk_values(zz, half):
        return jnp.concatenate([vbuf[zz, cc, half, xx] for cc in range(NC) for xx in range(NX)], axis=1)

    def score(work, t):
        zz, half, group = work
        s_ref[t] = jnp.dot(chunk_keys(zz, half), qt[group * 2 + t], preferred_element_type=jnp.float32)

    def accumulate(work, t, masked):
        zz, half, group = work
        p = group * 2 + t
        s = s_ref[t]
        if masked:
            r = lax.broadcasted_iota(jnp.int32, (CHUNK, NQ), 0)
            k_pos = ((r >> 6) & 1) * 512 + ((r >> 7) & 3) * 128 + (r >> 9) * 64 + (r & 63)
            q_pos = t * 512 + x * 128 + c * 64 + (lax.broadcasted_iota(jnp.int32, (CHUNK, NQ), 1) & 63)
            s = jnp.where(k_pos <= q_pos, s, NEG)
        m_old = m_ref[p]
        m_new = jnp.maximum(m_old, jnp.max(s, axis=0, keepdims=True))
        alpha = jnp.exp2(m_old - m_new)
        e = jnp.exp2(s - m_new)
        m_ref[p] = m_new
        l_ref[p] = l_ref[p] * alpha + jnp.sum(e, axis=0, keepdims=True)
        pv = jnp.dot(chunk_values(zz, half), e.astype(jnp.bfloat16), preferred_element_type=jnp.float32)
        o_ref[p] = o_ref[p] * alpha + pv

    def run(work, after, masked):
        score(work, 1)
        accumulate(work, 0, masked)
        if after is not None:
            score(after, 0)
        accumulate(work, 1, masked)

    def reaches(zz):
        return (zz <= z).astype(jnp.int32)

    def attend(zs, early=True):
        extra = 2 if early else 1
        n1 = 1 + extra * reaches(zs[0])
        total = n1 + (1 + extra * reaches(zs[1]) if len(zs) > 1 else 0)

        def decode(j):
            second = (j >= n1).astype(jnp.int32)
            zz = zs[0] + second * (zs[-1] - zs[0])
            jj = j - second * n1
            if not early:
                return zz, (jj == 1).astype(jnp.int32), 1
            return zz, (jj == 2).astype(jnp.int32), 1 - (jj == 0).astype(jnp.int32) * reaches(zz)

        score(decode(0), 0)

        def body(j, carry):
            run(decode(j), decode(jnp.minimum(j + 1, total - 1)), False)
            return carry

        lax.fori_loop(0, total, body, 0)

    def give_back(group):
        for t in (0, 1):
            p = group * 2 + t
            result = (o_ref[p] / l_ref[p]).T.astype(jnp.bfloat16)
            for h in range(REP):
                obuf[p, :, h * DH:(h + 1) * DH] = result[h * TOK:(h + 1) * TOK]

            @pl.when(y == p)
            def _(p=p):
                own_out(p).start()

            @pl.when(y != p)
            def _(p=p):
                piece(p).start()

    def own_out(p):
        return pltpu.make_async_copy(obuf.at[p], q_slice(out_hbm, y), local_sem.at[3])

    def piece(p):
        return remote(obuf.at[p], q_slice(out_hbm, y), sendo.at[p], recvo.at[y], device(x, p, z, c))

    crossed(z, 0)
    score((z, 0, 0), 0)
    run((z, 0, 0), (z, 0, 1), True)
    run((z, 0, 1), (z, 1, 1), False)
    run((z, 1, 1), None, True)
    for k in (1, 2, 3):
        advance_values(k + 1)
        advance_keys(k)
        for way, zz in ((0, low[k]), (1, high[k])):
            cross_values(zz, 2 * k - 1 + way)
        for way, zz in ((0, low[k]), (1, high[k])):
            crossed(zz, 2 * k - 1 + way)
        attend((low[k], high[k]))
    advance_keys(4)
    cross_values(far, 7)
    crossed(far, 7)

    @pl.when(far <= z)
    def _():
        score((far, 0, 0), 0)
        run((far, 0, 0), None, False)

    give_back(0)
    attend((far,), early=False)
    give_back(1)

    for p in range(NY):
        @pl.when(y == p)
        def _(p=p):
            own_out(p).wait()

        @pl.when(y != p)
        def _(p=p):
            remote(obuf.at[p], q_slice(out_hbm, p), sendo.at[p], recvo.at[p], partner).wait_recv()
            piece(p).wait_send()

    for cp in first_k + first_v + q_copies + started:
        cp.wait_send()


def per_device(queries, keys, values):
    bf16, f32 = jnp.bfloat16, jnp.float32
    dma = pltpu.SemaphoreType.DMA
    return pl.pallas_call(
        kernel,
        out_shape=jax.ShapeDtypeStruct(queries.shape, bf16),
        in_specs=[pl.BlockSpec(memory_space=pltpu.HBM)] * 3,
        out_specs=pl.BlockSpec(memory_space=pltpu.HBM),
        scratch_shapes=[
            pltpu.VMEM((NZ, NC, 2, NX, 2 * TOK, DH), bf16),
            pltpu.VMEM((NZ, NC, 2, NX, DH, 2 * TOK), bf16),
            pltpu.VMEM((2, 2 * TOK, DH), bf16),
            pltpu.VMEM((NY, TOK, COLS), bf16),
            pltpu.VMEM((NY, 2 * DH, NQ), bf16),
            pltpu.VMEM((NY, 1, NQ), f32),
            pltpu.VMEM((NY, 1, NQ), f32),
            pltpu.VMEM((NY, DH, NQ), f32),
            pltpu.VMEM((2, CHUNK, NQ), f32),
            pltpu.VMEM((NY, TOK, COLS), bf16),
            dma((2, 4)), dma((4,)), dma((4,)), dma((4,)), dma((4,)),
            dma((4,)), dma((4,)), dma((8, 4)), dma((8, 4)),
            dma((2, 2, 4)), dma((2, 2, 4)), dma((2, 8)), dma((2, 8)),
            dma((4,)), dma((4,)), dma((4,)),
        ],
        compiler_params=pltpu.CompilerParams(
            collective_id=0, has_side_effects=True, vmem_limit_bytes=60 * 2**20
        ),
        name="attention",
    )(queries, keys, values)


def solution(mesh):
    spec = P(("seq", "head"), None)
    return jax.shard_map(
        per_device, mesh=mesh, in_specs=(spec, spec, spec), out_specs=spec, check_vma=False
    )
```

```python
import functools
import math

import jax
import jax.numpy as jnp
from jax import lax
from jax.experimental import pallas as pl
from jax.experimental.pallas import tpu as pltpu
from jax.sharding import PartitionSpec as P

H = 32
KV = 4
DH = 128
NX, NY, NZ, NC = 4, 4, 8, 2
TOK = 64
REP = H // KV
COLS = REP * DH
NQ = REP * TOK
CHUNK = NX * NC * 2 * TOK
LOGICAL = pl.DeviceIdType.MESH
NEG = -1e30
FACTOR = math.log2(math.e) / math.sqrt(DH)


def device(x, y, z, c):
    return ((y // 2) * NZ + z, (y % 2) * (NX * NC) + x * NC + c)


def kernel(
    q_hbm, k_hbm, v_hbm, out_hbm,
    kbuf, vbuf, vloc, qin, qt, m_ref, l_ref, o_ref, s_ref, obuf,
    send0, recv0k, recv0v, sendq, recvq, sent, recvkx, recvvx,
    recvkz, recvvz, recvd, sendo, recvo, local_sem,
):
    seq, head = lax.axis_index("seq"), lax.axis_index("head")
    yh, z = seq // NZ, seq % NZ
    yl, x, c = head // (NX * NC), (head % (NX * NC)) // NC, head % NC
    y = yh * 2 + yl
    partner = device(x, y, z, 1 - c)
    right, left = device(x, y, (z + 1) % NZ, c), device(x, y, (z + NZ - 1) % NZ, c)
    low = [(z + NZ - k) % NZ for k in range(4)]
    high = [(z + k) % NZ for k in range(5)]
    far = high[4]

    def remote(src, dst, send, recv, dev):
        return pltpu.make_async_remote_copy(
            src_ref=src, dst_ref=dst, send_sem=send, recv_sem=recv,
            device_id=dev, device_id_type=LOGICAL,
        )

    @jax.named_scope("enter")
    def enter():
        for dev in peers:
            pl.semaphore_signal(barrier, inc=1, device_id=dev, device_id_type=LOGICAL)
        pl.semaphore_wait(barrier, len(peers))

    barrier = pltpu.get_barrier_semaphore()
    peers = [device(x, (y + d) % NY, z, c) for d in (1, 2, 3)]
    peers += [device((x + d) % NX, y, z, c) for d in (1, 2, 3)]
    peers += [right, left, partner]
    enter()

    def kv_slice(ref, g):
        return ref.at[:, pl.ds(pl.multiple_of(g * DH, DH), DH)]

    rows = pl.ds(pl.multiple_of(yl * TOK, TOK), TOK)
    first_k, first_v = [], []
    for d in (1, 3, 2):
        g = (y + d) % NY
        dev = device(x, g, z, c)
        first_v.append(remote(kv_slice(v_hbm, g), vloc.at[yh, rows], send0.at[0], recv0v.at[0], dev))
        first_k.append(remote(kv_slice(k_hbm, g), kbuf.at[z, c, yh, x, rows], send0.at[0], recv0k.at[0], dev))
    own_v = pltpu.make_async_copy(kv_slice(v_hbm, y), vloc.at[yh, rows], local_sem.at[1])
    own_k = pltpu.make_async_copy(kv_slice(k_hbm, y), kbuf.at[z, c, yh, x, rows], local_sem.at[0])
    for cp in first_v + [own_v] + first_k + [own_k]:
        cp.start()

    def q_slice(ref, g):
        return ref.at[:, pl.ds(pl.multiple_of(g * COLS, COLS), COLS)]

    q_copies = [
        remote(q_slice(q_hbm, (y + d) % NY), qin.at[y], sendq.at[0], recvq.at[0], device(x, (y + d) % NY, z, c))
        for d in (1, 3, 2)
    ]
    own_q = pltpu.make_async_copy(q_slice(q_hbm, y), qin.at[y], local_sem.at[2])
    for cp in q_copies + [own_q]:
        cp.start()

    def keys_x(h, d):
        part = kbuf.at[z, c, h, x]
        return remote(part, part, sent.at[3], recvkx.at[h], device((x + d) % NX, y, z, c))

    def keys_z(zz, step, way, h):
        part = kbuf.at[zz, c, h]
        kind = 2 if step < 3 else 3
        return remote(part, part, sent.at[kind], recvkz.at[step, h], right if way == 0 else left)

    def values_z(zz, step, way):
        part = vbuf.at[zz, c, :, x] if step < 3 else vbuf.at[zz, c, way, x]
        kind = 4 if step < 3 else 3
        return remote(part, part, sent.at[kind], recvvz.at[step], right if way == 0 else left)

    def values_x(zz, slot, h, d):
        part = vbuf.at[zz, c, h, x]
        return remote(part, part, sent.at[1], recvvx.at[slot, h], device((x + d) % NX, y, z, c))

    def across(a, zz, core, slot, h):
        part = (kbuf, vbuf)[a].at[zz, core, h]
        return remote(part, part, sent.at[0], recvd.at[(slot + 1) // 2, h], partner)

    def arrive(part, sem):
        remote(part, part, sent.at[0], sem, partner).wait_recv()

    def leave_by(part, sem):
        remote(part, part, sem, recvo.at[0], partner).wait_send()

    three, twelve = kbuf.at[0, 0, 0, 0:3], kbuf.at[0:3, 0, 0]

    def slots(k):
        return ((0, low[k], 2 * k - 1), (1, high[k], 2 * k)) if k < 4 else ((0, far, 7),)

    @jax.named_scope("spread_values")
    def spread_values(zz, slot, h):
        for d in (1, 3, 2):
            values_x(zz, slot, h, d).start()

    @jax.named_scope("cross_values")
    def cross_values(zz, slot, h):
        arrive(three, recvvx.at[slot, h])
        across(1, zz, c, slot, h).start()

    @jax.named_scope("settle")
    def settle(k, h):
        arrive(kbuf.at[0] if 0 < k < 4 else kbuf.at[0, 0], recvd.at[k, h])

    @jax.named_scope("advance_values")
    def advance_values(k):
        arrive(kbuf.at[0, 0, 0] if k < 4 else kbuf.at[0, 0, 0, 0:2], recvvz.at[k - 1])
        for way, zz, _ in slots(k):
            if k < 4:
                values_z(zz, k, way).start()
        for h in (0, 1):
            for _, zz, slot in slots(k):
                spread_values(zz, slot, h)

    @jax.named_scope("advance_keys")
    def advance_keys(k, h):
        arrive(kbuf.at[0, 0] if k < 4 else kbuf.at[0, 0, 0], recvkz.at[k - 1, h])
        for way, zz, slot in slots(k):
            if k < 3 or (k == 3 and way == h):
                keys_z(zz, k, way, h).start()
            across(0, zz, c, slot, h).start()

    with jax.named_scope("first"):
        own_v.wait()
        arrive(kbuf.at[0, 0, 0, 0:3, 0:TOK], recv0v.at[0])
    for h in (0, 1):
        vbuf[z, c, h, x] = vloc[h].astype(jnp.float32).T.astype(jnp.bfloat16)
    own_k.wait()
    arrive(kbuf.at[0, 0, 0, 0:3, 0:TOK], recv0k.at[0])
    for h in (0, 1):
        for d in (1, 3, 2):
            keys_x(h, d).start()
        if h == 0:
            for way in (0, 1):
                values_z(z, 0, way).start()
        spread_values(z, 0, h)

    m_ref[...] = jnp.full(m_ref.shape, NEG, jnp.float32)
    l_ref[...] = jnp.zeros(l_ref.shape, jnp.float32)
    o_ref[...] = jnp.zeros(o_ref.shape, jnp.float32)

    @jax.named_scope("begin")
    def begin(h):
        arrive(three, recvkx.at[h])
        for way in (0, 1):
            keys_z(z, 0, way, h).start()
        across(0, z, c, 0, h).start()

    advance_values(1)
    begin(0)
    cross_values(z, 0, 0)

    with jax.named_scope("queries"):
        own_q.wait()
        arrive(twelve, recvq.at[0])
        for p in range(NY):
            stacked = jnp.concatenate([qin[p, :, h * DH:(h + 1) * DH] for h in range(REP)], axis=0)
            scaled = (stacked.astype(jnp.float32) * FACTOR).T
            high_part = scaled.astype(jnp.bfloat16)
            qt[p, :DH] = high_part
            qt[p, DH:] = (scaled - high_part.astype(jnp.float32)).astype(jnp.bfloat16)

    def chunk_keys(zz, half):
        k = jnp.concatenate([kbuf[zz, cc, half, xx] for cc in range(NC) for xx in range(NX)], axis=0)
        return jnp.concatenate([k, k], axis=1)

    def chunk_values(zz, half):
        return jnp.concatenate([vbuf[zz, cc, half, xx] for cc in range(NC) for xx in range(NX)], axis=1)

    def score(work, t, place=None):
        zz, half, group = work
        s_ref[t if place is None else place] = jnp.dot(chunk_keys(zz, half), qt[group * 2 + t], preferred_element_type=jnp.float32)

    def accumulate(work, t, masked, place=None):
        zz, half, group = work
        p = group * 2 + t
        s = s_ref[t if place is None else place]
        if masked:
            r = lax.broadcasted_iota(jnp.int32, (CHUNK, NQ), 0)
            k_pos = ((r >> 6) & 1) * 512 + ((r >> 7) & 3) * 128 + (r >> 9) * 64 + (r & 63)
            q_pos = t * 512 + x * 128 + c * 64 + (lax.broadcasted_iota(jnp.int32, (CHUNK, NQ), 1) & 63)
            s = jnp.where(k_pos <= q_pos, s, NEG)
        m_old = m_ref[p]
        m_new = jnp.maximum(m_old, jnp.max(s, axis=0, keepdims=True))
        alpha = jnp.exp2(m_old - m_new)
        e = jnp.exp2(s - m_new)
        m_ref[p] = m_new
        wide = jnp.concatenate([chunk_values(zz, half), jnp.ones((16, CHUNK), jnp.bfloat16)], axis=0)
        pv = jnp.dot(wide, e.astype(jnp.bfloat16), preferred_element_type=jnp.float32)
        l_ref[p] = l_ref[p] * alpha + pv[DH:DH + 1]
        o_ref[p] = o_ref[p] * alpha + pv[:DH]

    def run(work, after, masked):
        score(work, 1)
        accumulate(work, 0, masked)
        if after is not None:
            score(after, 0)
        accumulate(work, 1, masked)

    def reaches(zz):
        return (zz <= z).astype(jnp.int32)

    def first_early(zz):
        return zz, 0, 1 - reaches(zz)

    def choose(flag, a, b):
        return tuple(v + flag * (w - v) for v, w in zip(a, b))

    @jax.named_scope("attend_early")
    def attend_early(zz, then, primed):
        total = 1 + reaches(zz)
        if not primed:
            score(first_early(zz), 0)

        def body(j, carry):
            last = (j == total - 1).astype(jnp.int32)
            run((zz, 0, last), choose(last, (zz, 0, 1), then), False)
            return carry

        lax.fori_loop(0, total, body, 0)

    @jax.named_scope("attend_late")
    def attend_late(a, b):
        total = reaches(a) + reaches(b)

        def body(j, carry):
            second = jnp.maximum(j, 1 - reaches(a))
            run((a + second * (b - a), 1, 1), (b, 1, 1), False)
            return carry

        lax.fori_loop(0, total, body, 0)

    @jax.named_scope("give_back")
    def give_back(p):
        result = (o_ref[p] / l_ref[p]).T.astype(jnp.bfloat16)
        for h in range(REP):
            obuf[p, :, h * DH:(h + 1) * DH] = result[h * TOK:(h + 1) * TOK]

        @pl.when(y == p)
        def _():
            own_out(p).start()

        @pl.when(y != p)
        def _():
            piece(p).start()

    def own_out(p):
        return pltpu.make_async_copy(obuf.at[p], q_slice(out_hbm, y), local_sem.at[3])

    def piece(p):
        return remote(obuf.at[p], q_slice(out_hbm, y), sendo.at[0], recvo.at[0], device(x, p, z, c))

    def cross_all(k, h):
        for _, zz, slot in slots(k):
            cross_values(zz, slot, h)

    settle(0, 0)
    with jax.named_scope("attend_own"):
        score((z, 0, 0), 0)
        run((z, 0, 0), (z, 0, 1), True)
    advance_values(2)
    begin(1)
    cross_values(z, 0, 1)
    with jax.named_scope("attend_own"):
        run((z, 0, 1), None, False)
    advance_keys(1, 0)
    settle(0, 1)
    with jax.named_scope("attend_own"):
        score((z, 1, 1), 0)
        run((z, 1, 1), None, True)
    cross_all(1, 0)
    advance_values(3)
    for k in (1, 2, 3):
        settle(k, 0)
        attend_early(low[k], first_early(high[k]), False)
        if k == 1:
            advance_keys(1, 1)
            cross_all(1, 1)
        else:
            advance_keys(k + 1, 0)
            cross_all(k + 1, 0)
            settle(k, 1)
        start_late = choose(reaches(low[k]), (high[k], 1, 1), (low[k], 1, 1))
        attend_early(high[k], (z, 1, 1) if k == 1 else start_late, True)
        if k == 1:
            advance_values(4)
            advance_keys(2, 0)
            cross_all(2, 0)
            settle(1, 1)
            score(start_late, 0)
        else:
            advance_keys(k + 1, 1)
            cross_all(k + 1, 1)
        if k < 3:
            attend_late(low[k], high[k])
        if k == 1:
            advance_keys(2, 1)
            cross_all(2, 1)
    odd = y % 2
    order = (1 - odd, odd, 3 - odd, 2 + odd)

    def steps(sequence):
        def item(n):
            zz, half, p = sequence[n]
            return (zz, half, p // 2), order[p] - 2 * (p // 2)

        def place(n):
            return n % 2

        for n in range(len(sequence) + 1):
            if n < len(sequence):
                work, t = item(n)
                score(work, t, place(n))
            if n > 0:
                work, t = item(n - 1)
                accumulate(work, t, False, place(n - 1))
                p = sequence[n - 1][2]
                if all(p != q for _, _, q in sequence[n:]):
                    give_back(order[p])

    full = z >= NZ - 3

    @pl.when(full)
    def _():
        settle(4, 0)
        settle(4, 1)
        rest = ((low[3], 1), (high[3], 1), (far, 0), (far, 1))
        steps([(far, 0, 0), (far, 0, 1)] + [(zz, half, p) for p in (2, 3) for zz, half in rest])

    @pl.when(jnp.logical_not(full))
    def _():
        attend_late(low[3], high[3])
        settle(4, 0)
        settle(4, 1)

        @pl.when(far <= z)
        def _():
            steps([(far, 0, 0), (far, 0, 1), (far, 0, 2), (far, 1, 2), (far, 0, 3), (far, 1, 3)])

        @pl.when(far > z)
        def _():
            give_back(order[0])
            give_back(order[1])
            steps([(far, 0, 2), (far, 0, 3)])

    with jax.named_scope("drain"):
        for kind, part in enumerate((kbuf, kbuf.at[0:3], kbuf.at[0:3], kbuf.at[0], twelve)):
            leave_by(part, sent.at[kind])
        leave_by(three, send0.at[0])
        leave_by(twelve, sendq.at[0])

    @jax.named_scope("leave")
    def leave():
        own_out(y).wait()
        arrive(twelve, recvo.at[0])
        leave_by(twelve, sendo.at[0])

    leave()


def per_device(queries, keys, values):
    bf16, f32 = jnp.bfloat16, jnp.float32
    dma = pltpu.SemaphoreType.DMA
    return pl.pallas_call(
        kernel,
        out_shape=jax.ShapeDtypeStruct(queries.shape, bf16),
        in_specs=[pl.BlockSpec(memory_space=pltpu.HBM)] * 3,
        out_specs=pl.BlockSpec(memory_space=pltpu.HBM),
        scratch_shapes=[
            pltpu.VMEM((NZ, NC, 2, NX, 2 * TOK, DH), bf16),
            pltpu.VMEM((NZ, NC, 2, NX, DH, 2 * TOK), bf16),
            pltpu.VMEM((2, 2 * TOK, DH), bf16),
            pltpu.VMEM((NY, TOK, COLS), bf16),
            pltpu.VMEM((NY, 2 * DH, NQ), bf16),
            pltpu.VMEM((NY, 1, NQ), f32),
            pltpu.VMEM((NY, 1, NQ), f32),
            pltpu.VMEM((NY, DH, NQ), f32),
            pltpu.VMEM((2, CHUNK, NQ), f32),
            pltpu.VMEM((NY, TOK, COLS), bf16),
            dma((1,)), dma((1,)), dma((1,)), dma((1,)), dma((1,)),
            dma((5,)), dma((2,)), dma((8, 2)), dma((4, 2)), dma((4,)), dma((5, 2)),
            dma((1,)), dma((1,)), dma((4,)),
        ],
        compiler_params=pltpu.CompilerParams(
            collective_id=0, has_side_effects=True, vmem_limit_bytes=60 * 2**20
        ),
        name="attention",
    )(queries, keys, values)


def solution(mesh):
    spec = P(("seq", "head"), None)
    return jax.shard_map(
        per_device, mesh=mesh, in_specs=(spec, spec, spec), out_specs=spec, check_vma=False
    )
```

```python
import functools
import math

import jax
import jax.numpy as jnp
from jax import lax
from jax.experimental import pallas as pl
from jax.experimental.pallas import tpu as pltpu
from jax.sharding import PartitionSpec as P

H = 32
KV = 4
DH = 128
NX, NY, NZ, NC = 4, 4, 8, 2
TOK = 64
REP = H // KV
COLS = REP * DH
NQ = REP * TOK
CHUNK = NX * NC * 2 * TOK
LOGICAL = pl.DeviceIdType.MESH
NEG = -1e30
FACTOR = math.log2(math.e) / math.sqrt(DH)


def device(x, y, z, c):
    return ((y // 2) * NZ + z, (y % 2) * (NX * NC) + x * NC + c)


def kernel(
    q_hbm, k_hbm, v_hbm, out_hbm,
    kbuf, vbuf, vloc, qin, qt, m_ref, l_ref, o_ref, s_ref, obuf,
    send0, recv0k, recv0v, sendq, recvq, sent, recvkx, recvvx,
    recvkz, recvvz, recvd, sendo, recvo, local_sem,
):
    seq, head = lax.axis_index("seq"), lax.axis_index("head")
    yh, z = seq // NZ, seq % NZ
    yl, x, c = head // (NX * NC), (head % (NX * NC)) // NC, head % NC
    y = yh * 2 + yl
    partner = device(x, y, z, 1 - c)
    right, left = device(x, y, (z + 1) % NZ, c), device(x, y, (z + NZ - 1) % NZ, c)
    low = [(z + NZ - k) % NZ for k in range(4)]
    high = [(z + k) % NZ for k in range(5)]
    far = high[4]

    def remote(src, dst, send, recv, dev):
        return pltpu.make_async_remote_copy(
            src_ref=src, dst_ref=dst, send_sem=send, recv_sem=recv,
            device_id=dev, device_id_type=LOGICAL,
        )

    @jax.named_scope("enter")
    def enter():
        for dev in peers:
            pl.semaphore_signal(barrier, inc=1, device_id=dev, device_id_type=LOGICAL)
        pl.semaphore_wait(barrier, len(peers))

    barrier = pltpu.get_barrier_semaphore()
    peers = [device(x, (y + d) % NY, z, c) for d in (1, 2, 3)]
    peers += [device((x + d) % NX, y, z, c) for d in (1, 2, 3)]
    peers += [right, left, partner]
    enter()

    def kv_slice(ref, g):
        return ref.at[:, pl.ds(pl.multiple_of(g * DH, DH), DH)]

    rows = pl.ds(pl.multiple_of(yl * TOK, TOK), TOK)
    first_k, first_v = [], []
    for d in (1, 3, 2):
        g = (y + d) % NY
        dev = device(x, g, z, c)
        first_v.append(remote(kv_slice(v_hbm, g), vloc.at[yh, rows], send0.at[0], recv0v.at[0], dev))
        first_k.append(remote(kv_slice(k_hbm, g), kbuf.at[z, c, yh, x, rows], send0.at[0], recv0k.at[0], dev))
    own_v = pltpu.make_async_copy(kv_slice(v_hbm, y), vloc.at[yh, rows], local_sem.at[1])
    own_k = pltpu.make_async_copy(kv_slice(k_hbm, y), kbuf.at[z, c, yh, x, rows], local_sem.at[0])
    for cp in first_v + [own_v] + first_k + [own_k]:
        cp.start()

    def q_slice(ref, g):
        return ref.at[:, pl.ds(pl.multiple_of(g * COLS, COLS), COLS)]

    q_copies = [
        remote(q_slice(q_hbm, (y + d) % NY), qin.at[y], sendq.at[0], recvq.at[0], device(x, (y + d) % NY, z, c))
        for d in (1, 3, 2)
    ]
    own_q = pltpu.make_async_copy(q_slice(q_hbm, y), qin.at[y], local_sem.at[2])
    for cp in q_copies + [own_q]:
        cp.start()

    def keys_x(h, d):
        part = kbuf.at[z, c, h, x]
        return remote(part, part, sent.at[3], recvkx.at[h], device((x + d) % NX, y, z, c))

    def keys_z(zz, step, way, h):
        part = kbuf.at[zz, c, h]
        kind = 2 if step < 3 else 3
        return remote(part, part, sent.at[kind], recvkz.at[step, h], right if way == 0 else left)

    def values_z(zz, step, way):
        part = vbuf.at[zz, c, :, x] if step < 3 else vbuf.at[zz, c, way, x]
        kind = 4 if step < 3 else 3
        return remote(part, part, sent.at[kind], recvvz.at[step], right if way == 0 else left)

    def values_x(zz, slot, h, d):
        part = vbuf.at[zz, c, h, x]
        return remote(part, part, sent.at[1], recvvx.at[slot, h], device((x + d) % NX, y, z, c))

    def across(a, zz, core, slot, h):
        part = (kbuf, vbuf)[a].at[zz, core, h]
        return remote(part, part, sent.at[0], recvd.at[(slot + 1) // 2, h], partner)

    def arrive(part, sem):
        remote(part, part, sent.at[0], sem, partner).wait_recv()

    def leave_by(part, sem):
        remote(part, part, sem, recvo.at[0], partner).wait_send()

    three, twelve = kbuf.at[0, 0, 0, 0:3], kbuf.at[0:3, 0, 0]

    def slots(k):
        return ((0, low[k], 2 * k - 1), (1, high[k], 2 * k)) if k < 4 else ((0, far, 7),)

    @jax.named_scope("spread_values")
    def spread_values(zz, slot, h):
        for d in (1, 3, 2):
            values_x(zz, slot, h, d).start()

    @jax.named_scope("cross_values")
    def cross_values(zz, slot, h):
        arrive(three, recvvx.at[slot, h])
        across(1, zz, c, slot, h).start()

    @jax.named_scope("settle")
    def settle(k, h):
        arrive(kbuf.at[0] if 0 < k < 4 else kbuf.at[0, 0], recvd.at[k, h])

    @jax.named_scope("advance_values")
    def advance_values(k, between=None):
        arrive(kbuf.at[0, 0, 0] if k < 4 else kbuf.at[0, 0, 0, 0:2], recvvz.at[k - 1])
        for way, zz, _ in slots(k):
            if k < 4:
                values_z(zz, k, way).start()
        if between is not None:
            between(1)
        for h in (0, 1):
            for _, zz, slot in slots(k):
                spread_values(zz, slot, h)

    @jax.named_scope("advance_keys")
    def advance_keys(k, h):
        arrive(kbuf.at[0, 0] if k < 4 else kbuf.at[0, 0, 0], recvkz.at[k - 1, h])
        for way, zz, slot in slots(k):
            if k < 3 or (k == 3 and way == h):
                keys_z(zz, k, way, h).start()
            across(0, zz, c, slot, h).start()

    with jax.named_scope("first"):
        own_v.wait()
        arrive(kbuf.at[0, 0, 0, 0:3, 0:TOK], recv0v.at[0])
    for h in (0, 1):
        vbuf[z, c, h, x] = vloc[h].astype(jnp.float32).T.astype(jnp.bfloat16)
    own_k.wait()
    arrive(kbuf.at[0, 0, 0, 0:3, 0:TOK], recv0k.at[0])
    def begin_x(h):
        for d in (1, 3, 2):
            keys_x(h, d).start()
        spread_values(z, 0, h)

    for way in (0, 1):
        values_z(z, 0, way).start()
    begin_x(0)

    m_ref[...] = jnp.full(m_ref.shape, NEG, jnp.float32)
    l_ref[...] = jnp.zeros(l_ref.shape, jnp.float32)
    o_ref[...] = jnp.zeros(o_ref.shape, jnp.float32)

    @jax.named_scope("begin")
    def begin(h):
        arrive(three, recvkx.at[h])
        for way in (0, 1):
            keys_z(z, 0, way, h).start()
        across(0, z, c, 0, h).start()

    advance_values(1, begin_x)
    begin(0)
    cross_values(z, 0, 0)

    with jax.named_scope("queries"):
        own_q.wait()
        arrive(twelve, recvq.at[0])
        for p in range(NY):
            stacked = jnp.concatenate([qin[p, :, h * DH:(h + 1) * DH] for h in range(REP)], axis=0)
            scaled = (stacked.astype(jnp.float32) * FACTOR).T
            high_part = scaled.astype(jnp.bfloat16)
            qt[p, :DH] = high_part
            qt[p, DH:] = (scaled - high_part.astype(jnp.float32)).astype(jnp.bfloat16)

    def chunk_keys(zz, half):
        k = jnp.concatenate([kbuf[zz, cc, half, xx] for cc in range(NC) for xx in range(NX)], axis=0)
        return jnp.concatenate([k, k], axis=1)

    def chunk_values(zz, half):
        return jnp.concatenate([vbuf[zz, cc, half, xx] for cc in range(NC) for xx in range(NX)], axis=1)

    def score(work, t, place=None):
        zz, half, group = work
        s_ref[t if place is None else place] = jnp.dot(chunk_keys(zz, half), qt[group * 2 + t], preferred_element_type=jnp.float32)

    def accumulate(work, t, masked, place=None):
        zz, half, group = work
        p = group * 2 + t
        s = s_ref[t if place is None else place]
        if masked:
            r = lax.broadcasted_iota(jnp.int32, (CHUNK, NQ), 0)
            k_pos = ((r >> 6) & 1) * 512 + ((r >> 7) & 3) * 128 + (r >> 9) * 64 + (r & 63)
            q_pos = t * 512 + x * 128 + c * 64 + (lax.broadcasted_iota(jnp.int32, (CHUNK, NQ), 1) & 63)
            s = jnp.where(k_pos <= q_pos, s, NEG)
        m_old = m_ref[p]
        m_new = jnp.maximum(m_old, jnp.max(s, axis=0, keepdims=True))
        alpha = jnp.exp2(m_old - m_new)
        e = jnp.exp2(s - m_new)
        m_ref[p] = m_new
        wide = jnp.concatenate([chunk_values(zz, half), jnp.ones((16, CHUNK), jnp.bfloat16)], axis=0)
        pv = jnp.dot(wide, e.astype(jnp.bfloat16), preferred_element_type=jnp.float32)
        l_ref[p] = l_ref[p] * alpha + pv[DH:DH + 1]
        o_ref[p] = o_ref[p] * alpha + pv[:DH]

    def run(work, after, masked):
        score(work, 1)
        accumulate(work, 0, masked)
        if after is not None:
            score(after, 0)
        accumulate(work, 1, masked)

    def reaches(zz):
        return (zz <= z).astype(jnp.int32)

    def first_early(zz):
        return zz, 0, 1 - reaches(zz)

    def choose(flag, a, b):
        return tuple(v + flag * (w - v) for v, w in zip(a, b))

    @jax.named_scope("attend_early")
    def attend_early(zz, then, primed):
        total = 1 + reaches(zz)
        if not primed:
            score(first_early(zz), 0)

        def body(j, carry):
            last = (j == total - 1).astype(jnp.int32)
            run((zz, 0, last), choose(last, (zz, 0, 1), then), False)
            return carry

        lax.fori_loop(0, total, body, 0)

    @jax.named_scope("attend_late")
    def attend_late(a, b):
        total = reaches(a) + reaches(b)

        def body(j, carry):
            second = jnp.maximum(j, 1 - reaches(a))
            run((a + second * (b - a), 1, 1), (b, 1, 1), False)
            return carry

        lax.fori_loop(0, total, body, 0)

    @jax.named_scope("give_back")
    def give_back(p):
        result = (o_ref[p] / l_ref[p]).T.astype(jnp.bfloat16)
        for h in range(REP):
            obuf[p, :, h * DH:(h + 1) * DH] = result[h * TOK:(h + 1) * TOK]

        @pl.when(y == p)
        def _():
            own_out(p).start()

        @pl.when(y != p)
        def _():
            piece(p).start()

    def own_out(p):
        return pltpu.make_async_copy(obuf.at[p], q_slice(out_hbm, y), local_sem.at[3])

    def piece(p):
        return remote(obuf.at[p], q_slice(out_hbm, y), sendo.at[0], recvo.at[0], device(x, p, z, c))

    def cross_all(k, h):
        for _, zz, slot in slots(k):
            cross_values(zz, slot, h)

    settle(0, 0)
    with jax.named_scope("attend_own"):
        score((z, 0, 0), 0)
        run((z, 0, 0), (z, 0, 1), True)
    advance_values(2)
    begin(1)
    cross_values(z, 0, 1)
    with jax.named_scope("attend_own"):
        run((z, 0, 1), None, False)
    advance_keys(1, 0)
    cross_all(1, 0)
    settle(0, 1)
    with jax.named_scope("attend_own"):
        score((z, 1, 1), 0)
        run((z, 1, 1), None, True)
    advance_values(3)
    for k in (1, 2, 3):
        settle(k, 0)
        attend_early(low[k], first_early(high[k]), False)
        if k == 1:
            advance_keys(1, 1)
            cross_all(1, 1)
        else:
            advance_keys(k + 1, 0)
            cross_all(k + 1, 0)
            settle(k, 1)
        start_late = choose(reaches(low[k]), (high[k], 1, 1), (low[k], 1, 1))
        attend_early(high[k], (z, 1, 1) if k == 1 else start_late, True)
        if k == 1:
            advance_values(4)
            advance_keys(2, 0)
            cross_all(2, 0)
            settle(1, 1)
            score(start_late, 0)
        else:
            advance_keys(k + 1, 1)
            cross_all(k + 1, 1)
        if k < 3:
            attend_late(low[k], high[k])
        if k == 1:
            advance_keys(2, 1)
            cross_all(2, 1)
    odd = y % 2
    order = (1 - odd, odd, 3 - odd, 2 + odd)

    def steps(sequence):
        def item(n):
            zz, half, p = sequence[n]
            return (zz, half, p // 2), order[p] - 2 * (p // 2)

        def place(n):
            return n % 2

        for n in range(len(sequence) + 1):
            if n < len(sequence):
                work, t = item(n)
                score(work, t, place(n))
            if n > 0:
                work, t = item(n - 1)
                accumulate(work, t, False, place(n - 1))
                p = sequence[n - 1][2]
                if all(p != q for _, _, q in sequence[n:]):
                    give_back(order[p])

    full = z >= NZ - 3

    @pl.when(full)
    def _():
        settle(4, 0)
        steps([(far, 0, 0), (far, 0, 1)])
        settle(4, 1)
        rest = ((low[3], 1), (high[3], 1), (far, 0), (far, 1))
        steps([(zz, half, p) for p in (2, 3) for zz, half in rest])

    @pl.when(jnp.logical_not(full))
    def _():
        attend_late(low[3], high[3])
        settle(4, 0)
        settle(4, 1)

        @pl.when(far <= z)
        def _():
            steps([(far, 0, 0), (far, 0, 1), (far, 0, 2), (far, 1, 2), (far, 0, 3), (far, 1, 3)])

        @pl.when(far > z)
        def _():
            give_back(order[0])
            give_back(order[1])
            steps([(far, 0, 2), (far, 0, 3)])

    with jax.named_scope("drain"):
        for kind, part in enumerate((kbuf, kbuf.at[0:3], kbuf.at[0:3], kbuf.at[0], twelve)):
            leave_by(part, sent.at[kind])
        leave_by(three, send0.at[0])
        leave_by(twelve, sendq.at[0])

    @jax.named_scope("leave")
    def leave():
        own_out(y).wait()
        arrive(twelve, recvo.at[0])
        leave_by(twelve, sendo.at[0])

    leave()


def per_device(queries, keys, values):
    bf16, f32 = jnp.bfloat16, jnp.float32
    dma = pltpu.SemaphoreType.DMA
    return pl.pallas_call(
        kernel,
        out_shape=jax.ShapeDtypeStruct(queries.shape, bf16),
        in_specs=[pl.BlockSpec(memory_space=pltpu.HBM)] * 3,
        out_specs=pl.BlockSpec(memory_space=pltpu.HBM),
        scratch_shapes=[
            pltpu.VMEM((NZ, NC, 2, NX, 2 * TOK, DH), bf16),
            pltpu.VMEM((NZ, NC, 2, NX, DH, 2 * TOK), bf16),
            pltpu.VMEM((2, 2 * TOK, DH), bf16),
            pltpu.VMEM((NY, TOK, COLS), bf16),
            pltpu.VMEM((NY, 2 * DH, NQ), bf16),
            pltpu.VMEM((NY, 1, NQ), f32),
            pltpu.VMEM((NY, 1, NQ), f32),
            pltpu.VMEM((NY, DH, NQ), f32),
            pltpu.VMEM((2, CHUNK, NQ), f32),
            pltpu.VMEM((NY, TOK, COLS), bf16),
            dma((1,)), dma((1,)), dma((1,)), dma((1,)), dma((1,)),
            dma((5,)), dma((2,)), dma((8, 2)), dma((4, 2)), dma((4,)), dma((5, 2)),
            dma((1,)), dma((1,)), dma((4,)),
        ],
        compiler_params=pltpu.CompilerParams(
            collective_id=0, has_side_effects=True, vmem_limit_bytes=60 * 2**20
        ),
        name="attention",
    )(queries, keys, values)


def solution(mesh):
    spec = P(("seq", "head"), None)
    return jax.shard_map(
        per_device, mesh=mesh, in_specs=(spec, spec, spec), out_specs=spec, check_vma=False
    )
```

```python
import functools
import math

import jax
import jax.numpy as jnp
from jax import lax
from jax.experimental import pallas as pl
from jax.experimental.pallas import tpu as pltpu
from jax.sharding import PartitionSpec as P

H = 32
KV = 4
DH = 128
NX, NY, NZ, NC = 4, 4, 8, 2
TOK = 64
REP = H // KV
COLS = REP * DH
NQ = REP * TOK
CHUNK = NX * NC * 2 * TOK
LOGICAL = pl.DeviceIdType.MESH
NEG = -1e30
FACTOR = math.log2(math.e) / math.sqrt(DH)


def device(x, y, z, c):
    return ((y // 2) * NZ + z, (y % 2) * (NX * NC) + x * NC + c)


def kernel(
    q_hbm, k_hbm, v_hbm, out_hbm,
    kbuf, vbuf, vloc, qin, qt, m_ref, l_ref, o_ref, s_ref, obuf,
    send0, recv0k, recv0v, sendq, recvq, sent, recvkx, recvvx,
    recvkz, recvvz, recvd, sendo, recvo, local_sem,
):
    seq, head = lax.axis_index("seq"), lax.axis_index("head")
    yh, z = seq // NZ, seq % NZ
    yl, x, c = head // (NX * NC), (head % (NX * NC)) // NC, head % NC
    y = yh * 2 + yl
    partner = device(x, y, z, 1 - c)
    right, left = device(x, y, (z + 1) % NZ, c), device(x, y, (z + NZ - 1) % NZ, c)
    low = [(z + NZ - k) % NZ for k in range(4)]
    high = [(z + k) % NZ for k in range(5)]
    far = high[4]

    def remote(src, dst, send, recv, dev):
        return pltpu.make_async_remote_copy(
            src_ref=src, dst_ref=dst, send_sem=send, recv_sem=recv,
            device_id=dev, device_id_type=LOGICAL,
        )

    @jax.named_scope("enter")
    def enter():
        for dev in peers:
            pl.semaphore_signal(barrier, inc=1, device_id=dev, device_id_type=LOGICAL)
        pl.semaphore_wait(barrier, len(peers))

    barrier = pltpu.get_barrier_semaphore()
    peers = [device(x, (y + d) % NY, z, c) for d in (1, 2, 3)]
    peers += [device((x + d) % NX, y, z, c) for d in (1, 2, 3)]
    peers = [right, left] + peers + [partner]
    enter()

    def kv_slice(ref, g):
        return ref.at[:, pl.ds(pl.multiple_of(g * DH, DH), DH)]

    rows = pl.ds(pl.multiple_of(yl * TOK, TOK), TOK)
    first_k, first_v = [], []
    for d in (1, 3, 2):
        g = (y + d) % NY
        dev = device(x, g, z, c)
        first_v.append(remote(kv_slice(v_hbm, g), vloc.at[yh, rows], send0.at[0], recv0v.at[0], dev))
        first_k.append(remote(kv_slice(k_hbm, g), kbuf.at[z, c, yh, x, rows], send0.at[0], recv0k.at[0], dev))
    own_v = pltpu.make_async_copy(kv_slice(v_hbm, y), vloc.at[yh, rows], local_sem.at[1])
    own_k = pltpu.make_async_copy(kv_slice(k_hbm, y), kbuf.at[z, c, yh, x, rows], local_sem.at[0])
    for cp in first_v + [own_v] + first_k + [own_k]:
        cp.start()

    def q_slice(ref, g):
        return ref.at[:, pl.ds(pl.multiple_of(g * COLS, COLS), COLS)]

    q_copies = [
        remote(q_slice(q_hbm, (y + d) % NY), qin.at[y], sendq.at[0], recvq.at[0], device(x, (y + d) % NY, z, c))
        for d in (1, 3, 2)
    ]
    own_q = pltpu.make_async_copy(q_slice(q_hbm, y), qin.at[y], local_sem.at[2])

    def keys_x(h, d):
        part = kbuf.at[z, c, h, x]
        return remote(part, part, sent.at[3], recvkx.at[h], device((x + d) % NX, y, z, c))

    def keys_z(zz, step, way, h):
        part = kbuf.at[zz, c, h]
        kind = 2 if step < 3 else 3
        return remote(part, part, sent.at[kind], recvkz.at[step, h], right if way == 0 else left)

    def values_z(zz, step, way):
        part = vbuf.at[zz, c, :, x] if step < 3 else vbuf.at[zz, c, way, x]
        kind = 4 if step < 3 else 3
        return remote(part, part, sent.at[kind], recvvz.at[step], right if way == 0 else left)

    def values_x(zz, slot, h, d):
        part = vbuf.at[zz, c, h, x]
        return remote(part, part, sent.at[1], recvvx.at[slot, h], device((x + d) % NX, y, z, c))

    def across(a, zz, core, slot, h):
        part = (kbuf, vbuf)[a].at[zz, core, h]
        return remote(part, part, sent.at[0], recvd.at[(slot + 1) // 2, h], partner)

    def arrive(part, sem):
        remote(part, part, sent.at[0], sem, partner).wait_recv()

    def leave_by(part, sem):
        remote(part, part, sem, recvo.at[0], partner).wait_send()

    three, twelve = kbuf.at[0, 0, 0, 0:3], kbuf.at[0:3, 0, 0]

    def slots(k):
        return ((0, low[k], 2 * k - 1), (1, high[k], 2 * k)) if k < 4 else ((0, far, 7),)

    @jax.named_scope("spread_values")
    def spread_values(zz, slot, h):
        for d in (1, 3, 2):
            values_x(zz, slot, h, d).start()

    @jax.named_scope("cross_values")
    def cross_values(zz, slot, h):
        arrive(three, recvvx.at[slot, h])
        across(1, zz, c, slot, h).start()

    @jax.named_scope("settle")
    def settle(k, h):
        arrive(kbuf.at[0] if 0 < k < 4 else kbuf.at[0, 0], recvd.at[k, h])

    @jax.named_scope("advance_values")
    def advance_values(k, between=None):
        arrive(kbuf.at[0, 0, 0] if k < 4 else kbuf.at[0, 0, 0, 0:2], recvvz.at[k - 1])
        for way, zz, _ in slots(k):
            if k < 4:
                values_z(zz, k, way).start()
        if between is not None:
            between(1)
        for h in (0, 1):
            for _, zz, slot in slots(k):
                spread_values(zz, slot, h)

    @jax.named_scope("advance_keys")
    def advance_keys(k, h):
        arrive(kbuf.at[0, 0] if k < 4 else kbuf.at[0, 0, 0], recvkz.at[k - 1, h])
        for way, zz, slot in slots(k):
            if k < 3 or (k == 3 and way == h):
                keys_z(zz, k, way, h).start()
            across(0, zz, c, slot, h).start()

    with jax.named_scope("first"):
        own_v.wait()
        arrive(kbuf.at[0, 0, 0, 0:3, 0:TOK], recv0v.at[0])
    for h in (0, 1):
        vbuf[z, c, h, x] = vloc[h].astype(jnp.float32).T.astype(jnp.bfloat16)
    own_k.wait()
    arrive(kbuf.at[0, 0, 0, 0:3, 0:TOK], recv0k.at[0])
    def begin_x(h):
        for d in (1, 3, 2):
            keys_x(h, d).start()
        spread_values(z, 0, h)

    for way in (0, 1):
        values_z(z, 0, way).start()
    begin_x(0)
    for cp in q_copies + [own_q]:
        cp.start()

    m_ref[...] = jnp.full(m_ref.shape, NEG, jnp.float32)
    l_ref[...] = jnp.zeros(l_ref.shape, jnp.float32)
    o_ref[...] = jnp.zeros(o_ref.shape, jnp.float32)

    @jax.named_scope("begin")
    def begin(h):
        arrive(three, recvkx.at[h])
        for way in (0, 1):
            keys_z(z, 0, way, h).start()
        across(0, z, c, 0, h).start()

    advance_values(1, begin_x)
    begin(0)
    cross_values(z, 0, 0)

    with jax.named_scope("queries"):
        own_q.wait()
        arrive(twelve, recvq.at[0])
        for p in range(NY):
            stacked = jnp.concatenate([qin[p, :, h * DH:(h + 1) * DH] for h in range(REP)], axis=0)
            scaled = (stacked.astype(jnp.float32) * FACTOR).T
            high_part = scaled.astype(jnp.bfloat16)
            qt[p, :DH] = high_part
            qt[p, DH:] = (scaled - high_part.astype(jnp.float32)).astype(jnp.bfloat16)

    def chunk_keys(zz, half):
        k = jnp.concatenate([kbuf[zz, cc, half, xx] for cc in range(NC) for xx in range(NX)], axis=0)
        return jnp.concatenate([k, k], axis=1)

    def chunk_values(zz, half):
        return jnp.concatenate([vbuf[zz, cc, half, xx] for cc in range(NC) for xx in range(NX)], axis=1)

    def score(work, t, place=None):
        zz, half, group = work
        s_ref[t if place is None else place] = jnp.dot(chunk_keys(zz, half), qt[group * 2 + t], preferred_element_type=jnp.float32)

    def accumulate(work, t, masked, place=None):
        zz, half, group = work
        p = group * 2 + t
        s = s_ref[t if place is None else place]
        if masked:
            r = lax.broadcasted_iota(jnp.int32, (CHUNK, NQ), 0)
            k_pos = ((r >> 6) & 1) * 512 + ((r >> 7) & 3) * 128 + (r >> 9) * 64 + (r & 63)
            q_pos = t * 512 + x * 128 + c * 64 + (lax.broadcasted_iota(jnp.int32, (CHUNK, NQ), 1) & 63)
            s = jnp.where(k_pos <= q_pos, s, NEG)
        m_old = m_ref[p]
        m_new = jnp.maximum(m_old, jnp.max(s, axis=0, keepdims=True))
        alpha = jnp.exp2(m_old - m_new)
        e = jnp.exp2(s - m_new)
        m_ref[p] = m_new
        wide = jnp.concatenate([chunk_values(zz, half), jnp.ones((16, CHUNK), jnp.bfloat16)], axis=0)
        pv = jnp.dot(wide, e.astype(jnp.bfloat16), preferred_element_type=jnp.float32)
        l_ref[p] = l_ref[p] * alpha + pv[DH:DH + 1]
        o_ref[p] = o_ref[p] * alpha + pv[:DH]

    def run(work, after, masked):
        score(work, 1)
        accumulate(work, 0, masked)
        if after is not None:
            score(after, 0)
        accumulate(work, 1, masked)

    def reaches(zz):
        return (zz <= z).astype(jnp.int32)

    def first_early(zz):
        return zz, 0, 1 - reaches(zz)

    def choose(flag, a, b):
        return tuple(v + flag * (w - v) for v, w in zip(a, b))

    @jax.named_scope("attend_early")
    def attend_early(zz, then, primed):
        total = 1 + reaches(zz)
        if not primed:
            score(first_early(zz), 0)

        def body(j, carry):
            last = (j == total - 1).astype(jnp.int32)
            run((zz, 0, last), choose(last, (zz, 0, 1), then), False)
            return carry

        lax.fori_loop(0, total, body, 0)

    @jax.named_scope("attend_late")
    def attend_late(a, b):
        total = reaches(a) + reaches(b)

        def body(j, carry):
            second = jnp.maximum(j, 1 - reaches(a))
            run((a + second * (b - a), 1, 1), (b, 1, 1), False)
            return carry

        lax.fori_loop(0, total, body, 0)

    @jax.named_scope("give_back")
    def give_back(p):
        result = (o_ref[p] / l_ref[p]).T.astype(jnp.bfloat16)
        for h in range(REP):
            obuf[p, :, h * DH:(h + 1) * DH] = result[h * TOK:(h + 1) * TOK]

        @pl.when(y == p)
        def _():
            own_out(p).start()

        @pl.when(y != p)
        def _():
            piece(p).start()

    def own_out(p):
        return pltpu.make_async_copy(obuf.at[p], q_slice(out_hbm, y), local_sem.at[3])

    def piece(p):
        return remote(obuf.at[p], q_slice(out_hbm, y), sendo.at[0], recvo.at[0], device(x, p, z, c))

    def cross_all(k, h):
        for _, zz, slot in slots(k):
            cross_values(zz, slot, h)

    settle(0, 0)
    with jax.named_scope("attend_own"):
        score((z, 0, 0), 0)
        run((z, 0, 0), (z, 0, 1), True)
    advance_values(2)
    begin(1)
    cross_values(z, 0, 1)
    with jax.named_scope("attend_own"):
        run((z, 0, 1), None, False)
    advance_keys(1, 0)
    cross_all(1, 0)
    settle(0, 1)
    with jax.named_scope("attend_own"):
        score((z, 1, 1), 0)
        run((z, 1, 1), None, True)
    advance_values(3)
    for k in (1, 2, 3):
        settle(k, 0)
        attend_early(low[k], first_early(high[k]), False)
        if k == 1:
            advance_keys(1, 1)
            cross_all(1, 1)
        else:
            advance_keys(k + 1, 0)
            cross_all(k + 1, 0)
            settle(k, 1)
        start_late = choose(reaches(low[k]), (high[k], 1, 1), (low[k], 1, 1))
        attend_early(high[k], (z, 1, 1) if k == 1 else start_late, True)
        if k == 1:
            advance_values(4)
            advance_keys(2, 0)
            cross_all(2, 0)
            settle(1, 1)
            score(start_late, 0)
        else:
            advance_keys(k + 1, 1)
            cross_all(k + 1, 1)
        if k < 3:
            attend_late(low[k], high[k])
        if k == 1:
            advance_keys(2, 1)
            cross_all(2, 1)
    odd = y % 2
    order = (1 - odd, odd, 3 - odd, 2 + odd)

    def steps(sequence):
        def item(n):
            zz, half, p = sequence[n]
            return (zz, half, p // 2), order[p] - 2 * (p // 2)

        def place(n):
            return n % 2

        for n in range(len(sequence) + 1):
            if n < len(sequence):
                work, t = item(n)
                score(work, t, place(n))
            if n > 0:
                work, t = item(n - 1)
                accumulate(work, t, False, place(n - 1))
                p = sequence[n - 1][2]
                if all(p != q for _, _, q in sequence[n:]):
                    give_back(order[p])

    full = z >= NZ - 3

    @pl.when(full)
    def _():
        settle(4, 0)
        steps([(far, 0, 0), (far, 0, 1)])
        settle(4, 1)
        rest = ((low[3], 1), (high[3], 1), (far, 0), (far, 1))
        steps([(zz, half, p) for p in (2, 3) for zz, half in rest])

    @pl.when(jnp.logical_not(full))
    def _():
        attend_late(low[3], high[3])
        settle(4, 0)
        settle(4, 1)

        @pl.when(far <= z)
        def _():
            steps([(far, 0, 0), (far, 0, 1), (far, 0, 2), (far, 1, 2), (far, 0, 3), (far, 1, 3)])

        @pl.when(far > z)
        def _():
            give_back(order[0])
            give_back(order[1])
            steps([(far, 0, 2), (far, 0, 3)])

    with jax.named_scope("drain"):
        for kind, part in enumerate((kbuf, kbuf.at[0:3], kbuf.at[0:3], kbuf.at[0], twelve)):
            leave_by(part, sent.at[kind])
        leave_by(three, send0.at[0])
        leave_by(twelve, sendq.at[0])

    @jax.named_scope("leave")
    def leave():
        own_out(y).wait()
        arrive(twelve, recvo.at[0])
        leave_by(twelve, sendo.at[0])

    leave()


def per_device(queries, keys, values):
    bf16, f32 = jnp.bfloat16, jnp.float32
    dma = pltpu.SemaphoreType.DMA
    return pl.pallas_call(
        kernel,
        out_shape=jax.ShapeDtypeStruct(queries.shape, bf16),
        in_specs=[pl.BlockSpec(memory_space=pltpu.HBM)] * 3,
        out_specs=pl.BlockSpec(memory_space=pltpu.HBM),
        scratch_shapes=[
            pltpu.VMEM((NZ, NC, 2, NX, 2 * TOK, DH), bf16),
            pltpu.VMEM((NZ, NC, 2, NX, DH, 2 * TOK), bf16),
            pltpu.VMEM((2, 2 * TOK, DH), bf16),
            pltpu.VMEM((NY, TOK, COLS), bf16),
            pltpu.VMEM((NY, 2 * DH, NQ), bf16),
            pltpu.VMEM((NY, 1, NQ), f32),
            pltpu.VMEM((NY, 1, NQ), f32),
            pltpu.VMEM((NY, DH, NQ), f32),
            pltpu.VMEM((2, CHUNK, NQ), f32),
            pltpu.VMEM((NY, TOK, COLS), bf16),
            dma((1,)), dma((1,)), dma((1,)), dma((1,)), dma((1,)),
            dma((5,)), dma((2,)), dma((8, 2)), dma((4, 2)), dma((4,)), dma((5, 2)),
            dma((1,)), dma((1,)), dma((4,)),
        ],
        compiler_params=pltpu.CompilerParams(
            collective_id=0, has_side_effects=True, vmem_limit_bytes=60 * 2**20
        ),
        name="attention",
    )(queries, keys, values)


def solution(mesh):
    spec = P(("seq", "head"), None)
    return jax.shard_map(
        per_device, mesh=mesh, in_specs=(spec, spec, spec), out_specs=spec, check_vma=False
    )
```
